128 devices in a mesh: depth: 16 (over z, y_hi, core), coef: 8 (over y_lo, x).
Axes of the slice: x: 4, y: 4 (y_hi: 2, y_lo: 2; y = y_hi * 2 + y_lo), z: 4, core: 2. Of those that a mesh axis runs over, the one named last changes fastest.
Arguments:
- volume: bfloat16 [64, 256, 64, 512], P('depth', None, 'coef'), may hold values from -1 to 1
- shift: int32 [64], P('depth'), may hold values from -64 to 64
- frac: int32 [64], P('depth'), may hold values from 0 to 16
- basis: bfloat16 [64, 64], replicated, may hold values from -0.75 to 0.75
- data: float32 [256, 64, 512], P(('depth', 'coef')), may hold values from 0.05 to 4
- mask: int32 [256, 64, 512], P(('depth', 'coef')), may hold values 0 or 1
Outputs:
- gradient: bfloat16 [64, 256, 64, 512], P('depth', None, 'coef')
- residual: bfloat16 [256, 64, 512], P(('depth', 'coef'))
The draws below stay inside these ranges and needn't reach their ends.
All inputs are finite; a program needn't handle non-finite values. No bound on the sum of `mask` on one device may be relied on, other than what follows from the above.
Results may differ from the reference program's by a relative error of at most 0.0053.
Values may be sent and summed in bfloat16 or wider, within the bound.
A program may use at most 128 MiB of HBM per device.

```python
import math
import jax
import jax.numpy as jnp
from jax import lax

X = 512
K = 64
G = 64
LAYERS = 64
Y = 256


def plant(drawn, rng, least, high):
    dims = drawn.shape
    spot = [jax.random.randint(jax.random.fold_in(rng, axis), (), 0, dims[axis]) for axis in range(len(dims))]
    drawn = drawn.at[tuple(spot)].set(least)
    longest = dims.index(max(dims))
    spot[longest] = (spot[longest] + 1) % dims[longest]
    return drawn.at[tuple(spot)].set(high)


def block_scale(key, extent, cuts, least, largest):
    def one(dim, shards_of):
        draws = jax.random.uniform(jax.random.fold_in(jax.random.fold_in(key, 6), dim), (shards_of,), jnp.float32, least / len(cuts), largest / len(cuts))
        return jnp.repeat(jnp.exp(draws), extent[dim] // shards_of).reshape((-1,) + (1,) * (len(extent) - dim - 1))

    factor_of = one(*cuts[0])
    for cut in cuts[1:]:
        factor_of = factor_of * one(*cut)
    return factor_of


def noise(rng, extent, spread, limit, shards=(), kind=jnp.bfloat16):
    gain = block_scale(rng, extent, shards, -0.22, 0.18) if shards else 1.0
    values = jax.random.normal(rng, extent, jnp.float32) * spread * gain
    return jnp.minimum(jnp.maximum(values, -limit), limit).astype(kind)


def setup_inputs(seed: int = 0) -> dict:
    seeds = jax.random.split(jax.random.key(seed), 7)
    volume = noise(seeds[0], (LAYERS, Y, K, X), 0.125, 1.0, ((0, 16), (2, 8)))
    shift = plant(jax.random.randint(seeds[1], (LAYERS,), 0 - X // 8, X // 8 + 1), jax.random.fold_in(seeds[1], 1), 0 - X // 8, (X // 8 + 1) - 1).astype(jnp.int32)
    frac = plant(jax.random.randint(seeds[2], (LAYERS,), 0, 17), jax.random.fold_in(seeds[2], 1), 0, 16).astype(jnp.int32)
    basis = noise(seeds[3], (K, G), K ** -0.5, 0.75)
    data = jnp.clip(jnp.exp(math.log(4.0) - 4.3820266 * jax.random.uniform(seeds[4], (Y, G, X), jnp.float32) ** block_scale(seeds[4], (Y, G, X), ((0, 128),), -0.2, 0.2)), 0.05, 4.0)
    mask = plant((jax.random.randint(seeds[5], (Y, G, X), 0, 4) < 3).astype(jnp.int32), jax.random.fold_in(seeds[5], 1), 0, 1)
    return {"volume": volume, "shift": shift, "frac": frac, "basis": basis, "data": data, "mask": mask}


def layer_tables(shift, frac, columns):
    position = jnp.arange(columns, dtype=jnp.int32)
    target = position[None, :, None] - shift.astype(jnp.int32)[:, None, None]
    weight = frac.astype(jnp.float32)[:, None, None] / 16.0
    column = position[None, None, :]
    matrix = jnp.where(column == target, 1.0 - weight, 0.0) + jnp.where(column == target - 1, weight, 0.0)
    return matrix.astype(jnp.bfloat16)

def reference(volume, shift, frac, basis, data, mask):
    interp = layer_tables(shift, frac, X)

    def accumulate(running, layer_pair):
        slab, matrix = layer_pair
        running = running + lax.dot_general(slab, matrix, (((2,), (1,)), ((), ())), preferred_element_type=jnp.float32)
        return (running, None)
    projection, _ = lax.scan(accumulate, jnp.zeros((Y, K, X), jnp.float32), (volume, interp))
    predicted = jnp.einsum('ykx,kg->ygx', projection, basis.astype(jnp.float32), precision=lax.Precision.HIGHEST)
    residual = (mask.astype(jnp.float32) * (predicted - jnp.sqrt(data))).astype(jnp.bfloat16)
    grad_proj = (2.0 * jnp.einsum('ygx,kg->ykx', residual.astype(jnp.float32), basis.astype(jnp.float32))).astype(jnp.bfloat16)

    def project_back(carry, matrix):
        slab = lax.dot_general(grad_proj, matrix, (((2,), (0,)), ((), ())), preferred_element_type=jnp.float32)
        return (carry, slab.astype(jnp.bfloat16))
    _, gradient = lax.scan(project_back, jnp.zeros((), jnp.float32), interp)
    return (gradient, residual)
```

```python
import functools

import jax
import jax.numpy as jnp
from jax import lax
from jax.experimental import pallas as pl
from jax.experimental.pallas import tpu as pltpu
from jax.sharding import PartitionSpec as P

MESH = pl.DeviceIdType.MESH
X = 512
LOCAL = 4
COEF = 8
BLOCK = 256
HALF = 128
PIECE = 16
ORDER = ((1, 0), (0, 1), (2, 0), (3, 1), (1, 1), (0, 0), (2, 1), (3, 0))


def place():
    d = lax.axis_index("depth")
    c = lax.axis_index("coef")
    return c % 4, c // 4, (d // 2) % 2, d // 4, d % 2


def device(x, yl, yh, z, core):
    return {"depth": z * 4 + yh * 2 + core, "coef": yl * 4 + x}


def exchange(
    vol, shift, frac, basis, basis_t, data, mask,
    grad_rows, resid,
    volbuf, interp, part, theirs, outgoing, incoming, total, wanted, valid, gp, gathered, res_buf,
    vol_sem, in_sem, pair_send, pair_recv, send_sem, recv_sem, back_send, back_recv,
    share_send, share_recv, out_sem,
):
    x, yl, yh, z, core = place()
    mine = yl * 4 + x
    partner = device(x, yl, yh, z, 1 - core)

    barrier = pltpu.get_barrier_semaphore()
    pl.semaphore_signal(barrier, inc=1, device_id=partner, device_id_type=MESH)
    for dz in range(4):
        for dyh in range(2):
            for dyl in range(2):
                for dx in range(4):
                    if dz or dyh or dyl or dx:
                        pl.semaphore_signal(
                            barrier,
                            inc=1,
                            device_id=device((x + dx) % 4, yl ^ dyl, yh ^ dyh, (z + dz) % 4, core),
                            device_id_type=MESH,
                        )

    loads = []
    for i, (dz, dyh) in enumerate(ORDER):
        block = ((z + dz) % 4) * 2 + (yh ^ dyh)
        load = pltpu.make_async_copy(
            vol.at[:, pl.ds(pl.multiple_of(block * BLOCK, BLOCK), BLOCK)], volbuf.at[i], vol_sem.at[i]
        )
        load.start()
        loads.append(load)
    load_data = pltpu.make_async_copy(data, wanted, in_sem.at[0])
    load_mask = pltpu.make_async_copy(mask, valid, in_sem.at[1])
    load_data.start()
    load_mask.start()

    for layer in range(LOCAL):
        s = shift[layer]
        w = frac[layer].astype(jnp.float32) * 0.0625

        def fill(t, carry, layer=layer, s=s, w=w):
            rows = t * HALF + lax.broadcasted_iota(jnp.int32, (HALF, X), 0)
            cols = lax.broadcasted_iota(jnp.int32, (HALF, X), 1)
            gap = cols - rows - s
            tile = jnp.where(gap == 0, 1.0 - w, jnp.where(gap == 1, w, 0.0))
            interp[layer, pl.ds(pl.multiple_of(t * HALF, HALF), HALF)] = tile.astype(jnp.bfloat16)
            return carry

        lax.fori_loop(0, X // HALF, fill, 0)

    for i in range(8):
        loads[i].wait()
        running = None
        for layer in range(LOCAL):
            slab = jnp.dot(volbuf[i, layer], interp[layer], preferred_element_type=jnp.float32)
            running = slab if running is None else running + slab
        part[i, 0] = running[:HALF]
        part[i, 1] = running[HALF:]

    pl.semaphore_wait(barrier, 64)

    shares = []
    for i in range(8):
        share = pltpu.make_async_remote_copy(
            part.at[i, 1 - core], theirs.at[i], pair_send.at[i], pair_recv.at[i],
            device_id=partner, device_id_type=MESH,
        )
        share.start()
        shares.append(share)

    load_data.wait()
    load_mask.wait()

    for i, (dz, dyh) in enumerate(ORDER):
        shares[i].wait_recv()
        outgoing[i] = (part[i, core] + theirs[i]).astype(jnp.bfloat16)
        for dyl in range(2):
            for dx in range(4):
                tyl, tx = yl ^ dyl, (x + dx) % 4
                source = outgoing.at[i, pl.ds(pl.multiple_of((tyl * 4 + tx) * PIECE, PIECE), PIECE)]
                target = incoming.at[i, pl.ds(pl.multiple_of(mine * PIECE, PIECE), PIECE)]
                if dz or dyh or dyl or dx:
                    pltpu.make_async_remote_copy(
                        source, target, send_sem.at[i], recv_sem.at[i],
                        device_id=device(tx, tyl, yh ^ dyh, (z + dz) % 4, core), device_id_type=MESH,
                    ).start()
                else:
                    keep = pltpu.make_async_copy(source, target, in_sem.at[2])
                    keep.start()

    for i in range(8):
        if ORDER[i] == (0, 0):
            keep.wait()
            pltpu.make_async_remote_copy(
                outgoing.at[i, pl.ds(0, 7 * PIECE)], incoming.at[i, pl.ds(0, 7 * PIECE)],
                send_sem.at[i], recv_sem.at[i], device_id=partner, device_id_type=MESH,
            ).wait_recv()
        else:
            pltpu.make_async_remote_copy(
                outgoing.at[i], incoming.at[i], send_sem.at[i], recv_sem.at[i],
                device_id=partner, device_id_type=MESH,
            ).wait_recv()
        if i == 0:
            total[...] = incoming[i].astype(jnp.float32)
        else:
            total[...] += incoming[i].astype(jnp.float32)

    sums = total[...].reshape(COEF, 2, COEF, X)
    slabs = []
    for r in range(2):
        proj = sums[:, r].reshape(64, X)
        high = proj.astype(jnp.bfloat16)
        low = (proj - high.astype(jnp.float32)).astype(jnp.bfloat16)
        predicted = jnp.dot(basis_t[...], high, preferred_element_type=jnp.float32) + jnp.dot(
            basis_t[...], low, preferred_element_type=jnp.float32
        )
        residual = (valid[r].astype(jnp.float32) * (predicted - jnp.sqrt(wanted[r]))).astype(jnp.bfloat16)
        res_buf[r] = residual
        slab = 2.0 * jnp.dot(basis[...], residual, preferred_element_type=jnp.float32)
        slabs.append(slab.reshape(COEF, COEF, X))
    gp[...] = jnp.stack(slabs, axis=1).reshape(HALF, X).astype(jnp.bfloat16)

    own_row = pl.multiple_of((z * 64 + yh * 32 + core * 16 + yl * 8 + x * 2) * COEF, PIECE)
    for i, (dz, dyh) in enumerate(ORDER):
        for dyl in range(2):
            for dx in range(4):
                tyl, tx = yl ^ dyl, (x + dx) % 4
                source = gp.at[pl.ds(pl.multiple_of((tyl * 4 + tx) * PIECE, PIECE), PIECE)]
                target = gathered.at[pl.ds(own_row, PIECE)]
                if dz or dyh or dyl or dx:
                    pltpu.make_async_remote_copy(
                        source, target, back_send.at[i], back_recv.at[i],
                        device_id=device(tx, tyl, yh ^ dyh, (z + dz) % 4, core), device_id_type=MESH,
                    ).start()
                else:
                    keep = pltpu.make_async_copy(source, target, in_sem.at[2])
                    keep.start()
    store_res = pltpu.make_async_copy(res_buf, resid, in_sem.at[0])
    store_res.start()

    passes = []
    for i, (dz, dyh) in enumerate(ORDER):
        block = ((z + 4 - dz) % 4) * 2 + (yh ^ dyh)
        rows = gathered.at[pl.ds(pl.multiple_of(block * BLOCK + core * HALF, HALF), HALF)]
        if dz or dyh:
            pltpu.make_async_remote_copy(
                gp, rows, back_send.at[i], back_recv.at[i], device_id=partner, device_id_type=MESH
            ).wait_recv()
        else:
            keep.wait()
            pltpu.make_async_remote_copy(
                gp.at[pl.ds(0, 7 * PIECE)],
                gathered.at[pl.ds(pl.multiple_of(block * BLOCK + core * HALF, HALF), 7 * PIECE)],
                back_send.at[i], back_recv.at[i], device_id=partner, device_id_type=MESH,
            ).wait_recv()
        onward = pltpu.make_async_remote_copy(
            rows, rows, share_send.at[i], share_recv.at[i], device_id=partner, device_id_type=MESH
        )
        onward.start()
        passes.append(onward)
    stores = []
    for i, (dz, dyh) in enumerate(ORDER):
        block = ((z + 4 - dz) % 4) * 2 + (yh ^ dyh)
        passes[i].wait_recv()
        span = pl.ds(pl.multiple_of(block * BLOCK, BLOCK), BLOCK)
        store = pltpu.make_async_copy(gathered.at[span], grad_rows.at[span], out_sem.at[i])
        store.start()
        stores.append(store)

    for i in range(8):
        shares[i].wait_send()
        count = 7 * PIECE if ORDER[i] == (0, 0) else HALF
        pltpu.make_async_remote_copy(
            outgoing.at[i, pl.ds(0, count)], incoming.at[i, pl.ds(0, count)],
            send_sem.at[i], recv_sem.at[i], device_id=partner, device_id_type=MESH,
        ).wait_send()
        pltpu.make_async_remote_copy(
            gp.at[pl.ds(0, count)], gathered.at[pl.ds(0, count)],
            back_send.at[i], back_recv.at[i], device_id=partner, device_id_type=MESH,
        ).wait_send()
        passes[i].wait_send()
    for store in stores:
        store.wait()
    store_res.wait()


def back_project(shift, frac, rows_ref, res_ref, grad_ref, res_out, interp):
    @pl.when(pl.program_id(0) == 0)
    def _():
        res_out[...] = res_ref[...]
        for layer in range(LOCAL):
            s = shift[layer]
            w = frac[layer].astype(jnp.float32) * 0.0625

            def fill(t, carry, layer=layer, s=s, w=w):
                rows = t * HALF + lax.broadcasted_iota(jnp.int32, (HALF, X), 0)
                cols = lax.broadcasted_iota(jnp.int32, (HALF, X), 1)
                gap = rows - cols - s
                tile = jnp.where(gap == 0, 1.0 - w, jnp.where(gap == 1, w, 0.0))
                interp[layer, pl.ds(pl.multiple_of(t * HALF, HALF), HALF)] = tile.astype(jnp.bfloat16)
                return carry

            lax.fori_loop(0, X // HALF, fill, 0)

    for layer in range(LOCAL):
        grad_ref[layer] = jnp.dot(
            rows_ref[...], interp[layer], preferred_element_type=jnp.float32
        ).astype(jnp.bfloat16)


def shards(volume, shift, frac, basis, data, mask):
    layers, rows, coefs, cols = volume.shape
    flat = rows * coefs
    vmem = pl.BlockSpec(memory_space=pltpu.VMEM)
    smem = pl.BlockSpec(memory_space=pltpu.SMEM)
    hbm = pl.BlockSpec(memory_space=pl.ANY)
    dma = pltpu.SemaphoreType.DMA
    grad_rows, resid = pl.pallas_call(
        exchange,
        out_shape=(
            jax.ShapeDtypeStruct((flat, cols), jnp.bfloat16),
            jax.ShapeDtypeStruct(data.shape, jnp.bfloat16),
        ),
        in_specs=[hbm, smem, smem, vmem, vmem, hbm, hbm],
        out_specs=(hbm, hbm),
        scratch_shapes=[
            pltpu.VMEM((8, layers, BLOCK, cols), jnp.bfloat16),
            pltpu.VMEM((layers, cols, cols), jnp.bfloat16),
            pltpu.VMEM((8, 2, HALF, cols), jnp.float32),
            pltpu.VMEM((8, HALF, cols), jnp.float32),
            pltpu.VMEM((8, HALF, cols), jnp.bfloat16),
            pltpu.VMEM((8, HALF, cols), jnp.bfloat16),
            pltpu.VMEM((HALF, cols), jnp.float32),
            pltpu.VMEM(data.shape, jnp.float32),
            pltpu.VMEM(mask.shape, jnp.int32),
            pltpu.VMEM((HALF, cols), jnp.bfloat16),
            pltpu.VMEM((flat, cols), jnp.bfloat16),
            pltpu.VMEM(data.shape, jnp.bfloat16),
            dma((8,)), dma((3,)), dma((8,)), dma((8,)), dma((8,)), dma((8,)), dma((8,)), dma((8,)),
            dma((8,)), dma((8,)), dma((8,)),
        ],
        compiler_params=pltpu.CompilerParams(
            collective_id=0, has_side_effects=True, vmem_limit_bytes=60 * 1024 * 1024
        ),
        name="exchange",
    )(volume.reshape(layers, flat, cols), shift, frac, basis, basis.T, data, mask)
    gradient, residual = pl.pallas_call(
        back_project,
        grid=(flat // BLOCK,),
        out_shape=(
            jax.ShapeDtypeStruct((layers, flat, cols), jnp.bfloat16),
            jax.ShapeDtypeStruct(data.shape, jnp.bfloat16),
        ),
        in_specs=[smem, smem, pl.BlockSpec((BLOCK, cols), lambda i: (i, 0)), pl.BlockSpec(data.shape, lambda i: (0, 0, 0))],
        out_specs=(
            pl.BlockSpec((layers, BLOCK, cols), lambda i: (0, i, 0)),
            pl.BlockSpec(data.shape, lambda i: (0, 0, 0)),
        ),
        scratch_shapes=[pltpu.VMEM((layers, cols, cols), jnp.bfloat16)],
        compiler_params=pltpu.CompilerParams(vmem_limit_bytes=24 * 1024 * 1024),
        name="back_project",
    )(shift, frac, grad_rows, resid)
    return gradient.reshape(volume.shape), residual


def solution(mesh):
    in_specs = (
        P("depth", None, "coef", None),
        P("depth"),
        P("depth"),
        P(),
        P(("depth", "coef"), None, None),
        P(("depth", "coef"), None, None),
    )
    out_specs = (P("depth", None, "coef", None), P(("depth", "coef"), None, None))
    return jax.shard_map(shards, mesh=mesh, in_specs=in_specs, out_specs=out_specs, check_vma=False)
```

```python
import functools

import jax
import jax.numpy as jnp
from jax import lax
from jax.experimental import pallas as pl
from jax.experimental.pallas import tpu as pltpu
from jax.sharding import PartitionSpec as P

MESH = pl.DeviceIdType.MESH
X = 512
LOCAL = 4
COEF = 8
BLOCK = 256
HALF = 128
PEERS = sorted(
    ((dz, dyh, dyl, dx) for dz in range(4) for dyh in range(2) for dyl in range(2) for dx in range(4))
)[:0:-1]
GROUPS = ((0, 4), (4, 2), (6, 2))
VMEM = 60 * 1024 * 1024
PIECES = 2
ORDER = ((1, 0), (0, 1), (2, 0), (3, 1), (1, 1), (0, 0), (2, 1), (3, 0))


def place():
    d = lax.axis_index("depth")
    c = lax.axis_index("coef")
    return c % 4, c // 4, (d // 2) % 2, d // 4, d % 2


def device(x, yl, yh, z, core):
    return {"depth": z * 4 + yh * 2 + core, "coef": yl * 4 + x}


def table(layer, shift, frac, band, corner, forward):
    s = shift[layer]
    w = frac[layer].astype(jnp.float32) * 0.0625
    rows = lax.broadcasted_iota(jnp.int32, (BLOCK, BLOCK), 0)
    cols = lax.broadcasted_iota(jnp.int32, (BLOCK, BLOCK), 1)
    gap = (cols - rows if forward else rows - cols) - s
    tile = jnp.where(gap == 0, 1.0 - w, jnp.where(gap == 1, w, 0.0)).astype(jnp.bfloat16)
    empty = jnp.zeros((HALF, HALF), jnp.bfloat16)
    span = pl.ds(layer * BLOCK, BLOCK)
    band[span] = tile
    corner[span] = jnp.concatenate(
        [
            jnp.concatenate([empty, tile[:HALF, HALF:]], axis=1),
            jnp.concatenate([tile[HALF:, :HALF], empty], axis=1),
        ],
        axis=0,
    )


def banded(lanes, band, corner):
    low, middle, high = lanes(0), lanes(HALF), lanes(BLOCK)
    m = low.shape[0]
    sides = jnp.dot(jnp.concatenate([low, high], axis=0), band, preferred_element_type=jnp.float32)
    inner = jnp.dot(middle, corner, preferred_element_type=jnp.float32)
    return (
        sides[:m, :HALF],
        sides[:m, HALF:] + inner[:, :HALF],
        sides[m:, :HALF] + inner[:, HALF:],
        sides[m:, HALF:],
    )


def exchange(
    vol, shift_hbm, frac_hbm, basis, data, mask,
    grad_rows, tables, resid,
    volbuf, shift, frac, band, corner, back_band, back_corner, gathered, res_buf, part, theirs, outgoing, incoming, total, wanted, valid, mix, gp,
    vol_sem, in_sem, self_sem, pair_send, pair_recv, send_sem, recv_sem, back_send, back_recv,
    share_send, share_recv, out_sem,
):
    x, yl, yh, z, core = place()
    mine = yl * 4 + x
    partner = device(x, yl, yh, z, 1 - core)

    def remote(source, target, send, recv, to=partner):
        return pltpu.make_async_remote_copy(source, target, send, recv, device_id=to, device_id_type=MESH)

    words = [
        pltpu.make_async_copy(shift_hbm, shift, in_sem.at[3]),
        pltpu.make_async_copy(frac_hbm, frac, in_sem.at[4]),
    ]
    for load in words:
        load.start()
    loads = []
    for i, (dz, dyh) in enumerate(ORDER):
        block = ((z + dz) % 4) * 2 + (yh ^ dyh)
        load = pltpu.make_async_copy(
            vol.at[:, pl.ds(pl.multiple_of(block * BLOCK, BLOCK), BLOCK)], volbuf.at[i], vol_sem.at[i]
        )
        load.start()
        loads.append(load)
    barrier = pltpu.get_barrier_semaphore()
    for dz, dyh, dyl, dx in PEERS:
        to = device((x + dx) % 4, yl ^ dyl, yh ^ dyh, (z + dz) % 4, core)
        pl.semaphore_signal(barrier, inc=1, device_id=to, device_id_type=MESH)
    pl.semaphore_signal(barrier, inc=1, device_id=partner, device_id_type=MESH)

    small = [
        pltpu.make_async_copy(data, wanted, in_sem.at[0]),
        pltpu.make_async_copy(mask, valid, in_sem.at[1]),
        pltpu.make_async_copy(basis, mix, in_sem.at[2]),
    ]
    for load in small:
        load.start()

    for load in words:
        load.wait()
    for layer in range(LOCAL):
        table(layer, shift, frac, band, corner, True)

    def compute(first, count):
        for i in range(first, first + count):
            loads[i].wait()

        def lanes(low):
            return jnp.concatenate(
                [
                    volbuf[first : first + count, layer, :, low : low + BLOCK].reshape(count * BLOCK, BLOCK)
                    for layer in range(LOCAL)
                ],
                axis=1,
            )

        for q, piece in enumerate(banded(lanes, band[...], corner[...])):
            part[first : first + count, :, :, :, :, q * HALF : (q + 1) * HALF] = piece.reshape(
                count, 2, COEF, 2, COEF, HALF
            )

    shares = [remote(part.at[i, 1 - core], theirs.at[i], pair_send.at[i], pair_recv.at[i]) for i in range(8)]

    def is_self(i, dyl, dx):
        return ORDER[i] == (0, 0) and dyl == 0 and dx == 0

    def dispatch(r, i):
        dz, dyh = ORDER[i]
        if r == 0:
            shares[i].wait_recv()
        outgoing[r, i] = (part[i, core, :, r] + theirs[i, :, r]).astype(jnp.bfloat16)
        for dyl in range(2):
            for dx in range(4):
                tyl, tx = yl ^ dyl, (x + dx) % 4
                source = outgoing.at[r, i, tyl * 4 + tx]
                target = incoming.at[r, i, mine]
                if is_self(i, dyl, dx):
                    pltpu.make_async_copy(source, target, self_sem.at[r]).start()
                else:
                    to = device(tx, tyl, yh ^ dyh, (z + dz) % 4, core)
                    remote(source, target, send_sem.at[r, i], recv_sem.at[r, i], to).start()

    done, ready = 0, 0
    for first, count in GROUPS:
        compute(first, count)
        if first == 0:
            pl.semaphore_wait(barrier, 64)
        for i in range(first, first + count):
            shares[i].start()
        while done < ready:
            dispatch(0, done)
            done += 1
        ready = first + count
    while done < 8:
        dispatch(0, done)
        done += 1
    for i in range(8):
        dispatch(1, i)

    for layer in range(LOCAL):
        table(layer, shift, frac, back_band, back_corner, False)
    store_tables = [
        pltpu.make_async_copy(back_band, tables.at[0], in_sem.at[3]),
        pltpu.make_async_copy(back_corner, tables.at[1], in_sem.at[4]),
    ]
    for store in store_tables:
        store.start()
    for load in small:
        load.wait()
    turned = mix[...].astype(jnp.float32).T.astype(jnp.bfloat16)

    for r in range(2):
        for i in range(8):
            count = 8
            if ORDER[i] == (0, 0):
                pltpu.make_async_copy(outgoing.at[r, i, 0], incoming.at[r, i, 0], self_sem.at[r]).wait()
                count = 7
            remote(
                outgoing.at[r, i, pl.ds(0, count)], incoming.at[r, i, pl.ds(0, count)],
                send_sem.at[r, i], recv_sem.at[r, i],
            ).wait_recv()
            piece = incoming[r, i].astype(jnp.float32).reshape(64, X)
            if i == 0:
                total[r] = piece
            else:
                total[r] += piece
        proj = total[r]
        high = proj.astype(jnp.bfloat16)
        low = (proj - high.astype(jnp.float32)).astype(jnp.bfloat16)
        predicted = jnp.dot(turned, high, preferred_element_type=jnp.float32) + jnp.dot(
            turned, low, preferred_element_type=jnp.float32
        )
        residual = (valid[r].astype(jnp.float32) * (predicted - jnp.sqrt(wanted[r]))).astype(jnp.bfloat16)
        res_buf[r] = residual
        slab = 2.0 * jnp.dot(mix[...], residual, preferred_element_type=jnp.float32)
        gp[r] = slab.reshape(COEF, COEF, X).astype(jnp.bfloat16)
        for i, (dz, dyh) in enumerate(ORDER):
            for dyl in range(2):
                for dx in range(4):
                    tyl, tx = yl ^ dyl, (x + dx) % 4
                    source = gp.at[r, tyl * 4 + tx]
                    target = gathered.at[z * 2 + yh, mine, r]
                    if is_self(i, dyl, dx):
                        pltpu.make_async_copy(source, target, self_sem.at[r]).start()
                    else:
                        to = device(tx, tyl, yh ^ dyh, (z + dz) % 4, core)
                        remote(source, target, back_send.at[r, i], back_recv.at[r, i], to).start()

    store_res = pltpu.make_async_copy(res_buf, resid, in_sem.at[0])
    store_res.start()
    passes = []
    for r in range(2):
        for i, (dz, dyh) in enumerate(ORDER):
            block = ((z + 4 - dz) % 4) * 2 + (yh ^ dyh)
            rows = gathered.at[block, :, r]
            count = 8
            if ORDER[i] == (0, 0):
                pltpu.make_async_copy(gp.at[r, 0], gathered.at[block, 0, r], self_sem.at[r]).wait()
                count = 7
            remote(
                gp.at[r, pl.ds(0, count)], gathered.at[block, pl.ds(0, count), r],
                back_send.at[r, i], back_recv.at[r, i],
            ).wait_recv()
            home = grad_rows.at[block, core, :, r]
            onward = remote(rows, home, share_send.at[r, i], share_recv.at[r, i])
            onward.start()
            store = pltpu.make_async_copy(rows, home, out_sem.at[r, i])
            store.start()
            passes += [onward, store]
    for store in passes + store_tables + [store_res]:
        store.wait()
    for i in range(8):
        shares[i].wait_send()
        count = 7 if ORDER[i] == (0, 0) else 8
        for r in range(2):
            remote(
                outgoing.at[r, i, pl.ds(0, count)], incoming.at[r, i, pl.ds(0, count)],
                send_sem.at[r, i], recv_sem.at[r, i],
            ).wait_send()
            remote(
                gp.at[r, pl.ds(0, count)], incoming.at[r, i, pl.ds(0, count)],
                back_send.at[r, i], back_recv.at[r, i],
            ).wait_send()


def back_project(rows_hbm, tables_hbm, res_in, grad, res_out, rows_ref, tables, res_buf, staged, load_sem, sem):
    size = rows_ref.shape[1]
    loads = [pltpu.make_async_copy(tables_hbm, tables, load_sem.at[0])]
    for t in range(PIECES):
        loads.append(pltpu.make_async_copy(rows_hbm.at[pl.ds(t * size, size)], rows_ref.at[t], load_sem.at[t + 1]))
    last = pltpu.make_async_copy(res_in, res_buf, load_sem.at[PIECES + 1])
    for load in loads + [last]:
        load.start()
    loads[0].wait()
    stores = []
    for t in range(PIECES):
        loads[t + 1].wait()
        for layer in range(LOCAL):
            span = slice(layer * BLOCK, (layer + 1) * BLOCK)
            pieces = banded(lambda low: rows_ref[t, :, low : low + BLOCK], tables[0, span], tables[1, span])
            for q, piece in enumerate(pieces):
                staged[t, layer, :, q * HALF : (q + 1) * HALF] = piece.astype(jnp.bfloat16)
            store = pltpu.make_async_copy(
                staged.at[t, layer], grad.at[layer, pl.ds(t * size, size)], sem.at[t * LOCAL + layer]
            )
            store.start()
            stores.append(store)
        if t == 0:
            last.wait()
            keep = pltpu.make_async_copy(res_buf, res_out, load_sem.at[0])
            keep.start()
            stores.append(keep)
    for store in stores:
        store.wait()


def shards(volume, shift, frac, basis, data, mask):
    layers, rows, coefs, cols = volume.shape
    flat = rows * coefs
    hbm = pl.BlockSpec(memory_space=pl.ANY)
    dma = pltpu.SemaphoreType.DMA
    tall = layers * BLOCK
    grad_rows, tables, resid = pl.pallas_call(
        exchange,
        out_shape=(
            jax.ShapeDtypeStruct((8, 2, 8, 2, coefs, cols), jnp.bfloat16),
            jax.ShapeDtypeStruct((2, tall, BLOCK), jnp.bfloat16),
            jax.ShapeDtypeStruct(data.shape, jnp.bfloat16),
        ),
        in_specs=[hbm] * 6,
        out_specs=(hbm, hbm, hbm),
        scratch_shapes=[
            pltpu.VMEM((8, layers, BLOCK, cols), jnp.bfloat16),
            pltpu.SMEM(shift.shape, jnp.int32),
            pltpu.SMEM(frac.shape, jnp.int32),
            pltpu.VMEM((tall, BLOCK), jnp.bfloat16),
            pltpu.VMEM((tall, BLOCK), jnp.bfloat16),
            pltpu.VMEM((tall, BLOCK), jnp.bfloat16),
            pltpu.VMEM((tall, BLOCK), jnp.bfloat16),
            pltpu.VMEM((8, 8, 2, coefs, cols), jnp.bfloat16),
            pltpu.VMEM(data.shape, jnp.bfloat16),
            pltpu.VMEM((8, 2, 8, 2, coefs, cols), jnp.float32),
            pltpu.VMEM((8, 8, 2, coefs, cols), jnp.float32),
            pltpu.VMEM((2, 8, 8, coefs, cols), jnp.bfloat16),
            pltpu.VMEM((2, 8, 8, coefs, cols), jnp.bfloat16),
            pltpu.VMEM((2, 64, cols), jnp.float32),
            pltpu.VMEM(data.shape, jnp.float32),
            pltpu.VMEM(mask.shape, jnp.int32),
            pltpu.VMEM(basis.shape, jnp.bfloat16),
            pltpu.VMEM((2, 8, coefs, cols), jnp.bfloat16),
            dma((8,)), dma((5,)), dma((2,)), dma((8,)), dma((8,)), dma((2, 8)), dma((2, 8)),
            dma((2, 8)), dma((2, 8)), dma((2, 8)), dma((2, 8)), dma((2, 8)),
        ],
        compiler_params=pltpu.CompilerParams(collective_id=0, has_side_effects=True, vmem_limit_bytes=VMEM),
        name="exchange",
    )(volume.reshape(layers, flat, cols), shift, frac, basis, data, mask)
    gradient, residual = pl.pallas_call(
        back_project,
        out_shape=(
            jax.ShapeDtypeStruct((layers, flat, cols), jnp.bfloat16),
            jax.ShapeDtypeStruct(data.shape, jnp.bfloat16),
        ),
        in_specs=[hbm] * 3,
        out_specs=(hbm, hbm),
        scratch_shapes=[
            pltpu.VMEM((PIECES, flat // PIECES, cols), jnp.bfloat16),
            pltpu.VMEM((2, tall, BLOCK), jnp.bfloat16),
            pltpu.VMEM(data.shape, jnp.bfloat16),
            pltpu.VMEM((PIECES, layers, flat // PIECES, cols), jnp.bfloat16),
            dma((PIECES + 2,)),
            dma((PIECES * layers,)),
        ],
        compiler_params=pltpu.CompilerParams(vmem_limit_bytes=VMEM),
        name="back_project",
    )(grad_rows.reshape(flat, cols), tables, resid)
    return gradient.reshape(volume.shape), residual


def solution(mesh):
    in_specs = (
        P("depth", None, "coef", None),
        P("depth"),
        P("depth"),
        P(),
        P(("depth", "coef"), None, None),
        P(("depth", "coef"), None, None),
    )
    out_specs = (P("depth", None, "coef", None), P(("depth", "coef"), None, None))
    return jax.shard_map(shards, mesh=mesh, in_specs=in_specs, out_specs=out_specs, check_vma=False)
```

```python
import functools

import jax
import jax.numpy as jnp
from jax import lax
from jax.experimental import pallas as pl
from jax.experimental.pallas import tpu as pltpu
from jax.sharding import PartitionSpec as P

MESH = pl.DeviceIdType.MESH
X = 512
LOCAL = 4
COEF = 8
BLOCK = 256
HALF = 128
PEERS = sorted(
    ((dz, dyh, dyl, dx) for dz in range(4) for dyh in range(2) for dyl in range(2) for dx in range(4)),
    key=lambda p: min(p[0], 4 - p[0]) + (1 if p[2] else 2 * p[1]) + min(p[3], 4 - p[3]),
)[:0:-1]
GROUPS = ((0, 4), (4, 2), (6, 2))
VMEM = 60 * 1024 * 1024
PIECES = 4
ORDER = ((1, 0), (0, 1), (2, 0), (3, 1), (1, 1), (2, 1), (3, 0), (0, 0))
KEPT = tuple(7 if pair == (0, 0) else 8 for pair in ORDER)


def place():
    d = lax.axis_index("depth")
    c = lax.axis_index("coef")
    return c % 4, c // 4, (d // 2) % 2, d // 4, d % 2


def device(x, yl, yh, z, core):
    return {"depth": z * 4 + yh * 2 + core, "coef": yl * 4 + x}


def table(layer, shift, frac, band, corner):
    s = shift[layer]
    w = frac[layer].astype(jnp.float32) * 0.0625
    rows = lax.broadcasted_iota(jnp.int32, (BLOCK, BLOCK), 0)
    cols = lax.broadcasted_iota(jnp.int32, (BLOCK, BLOCK), 1)
    gap = cols - rows - s
    tile = jnp.where(gap == 0, 1.0 - w, jnp.where(gap == 1, w, 0.0)).astype(jnp.bfloat16)
    empty = jnp.zeros((HALF, HALF), jnp.bfloat16)
    span = pl.ds(layer * BLOCK, BLOCK)
    band[span] = tile
    corner[span] = jnp.concatenate(
        [
            jnp.concatenate([empty, tile[:HALF, HALF:]], axis=1),
            jnp.concatenate([tile[HALF:, :HALF], empty], axis=1),
        ],
        axis=0,
    )


def back_table(shift, frac, pair):
    rows = lax.broadcasted_iota(jnp.int32, (BLOCK, HALF), 0)
    cols = lax.broadcasted_iota(jnp.int32, (BLOCK, HALF), 1)
    halves = []
    for layer in (2 * pair, 2 * pair + 1):
        s = shift[layer]
        w = frac[layer].astype(jnp.float32) * 0.0625
        gap = rows - cols - jnp.where(s < 0, s + HALF, s)
        halves.append(jnp.where(gap == 0, 1.0 - w, jnp.where(gap == 1, w, 0.0)).astype(jnp.bfloat16))
    return jnp.concatenate(halves, axis=1)


def banded(lanes, band, corner):
    low, middle, high = lanes(0), lanes(HALF), lanes(BLOCK)
    m = low.shape[0]
    sides = jnp.dot(jnp.concatenate([low, high], axis=0), band, preferred_element_type=jnp.float32)
    inner = jnp.dot(middle, corner, preferred_element_type=jnp.float32)
    return (
        sides[:m, :HALF],
        sides[:m, HALF:] + inner[:, :HALF],
        sides[m:, :HALF] + inner[:, HALF:],
        sides[m:, HALF:],
    )


def exchange(
    vol, shift_hbm, frac_hbm, basis, data, mask,
    grad_rows, tables, resid,
    volbuf, shift, frac, band, corner, back, gathered, res_buf, part, theirs, outgoing, incoming, total, wanted, valid, mix, gp,
    vol_sem, in_sem, self_sem, pair_send, pair_recv, send_sem, recv_sem, back_send, back_recv,
    share_send, share_recv, out_sem,
):
    x, yl, yh, z, core = place()
    mine = yl * 4 + x
    partner = device(x, yl, yh, z, 1 - core)

    def remote(source, target, send, recv, to=partner):
        return pltpu.make_async_remote_copy(source, target, send, recv, device_id=to, device_id_type=MESH)

    words = [
        pltpu.make_async_copy(shift_hbm, shift, in_sem.at[3]),
        pltpu.make_async_copy(frac_hbm, frac, in_sem.at[4]),
    ]
    for load in words:
        load.start()
    loads = []
    for i, (dz, dyh) in enumerate(ORDER):
        block = ((z + dz) % 4) * 2 + (yh ^ dyh)
        load = pltpu.make_async_copy(
            vol.at[:, pl.ds(pl.multiple_of(block * BLOCK, BLOCK), BLOCK)], volbuf.at[i], vol_sem.at[i]
        )
        load.start()
        loads.append(load)
    barrier = pltpu.get_barrier_semaphore()
    for dz, dyh, dyl, dx in PEERS:
        to = device((x + dx) % 4, yl ^ dyl, yh ^ dyh, (z + dz) % 4, core)
        pl.semaphore_signal(barrier, inc=1, device_id=to, device_id_type=MESH)
    pl.semaphore_signal(barrier, inc=1, device_id=partner, device_id_type=MESH)

    small = [
        pltpu.make_async_copy(data, wanted, in_sem.at[0]),
        pltpu.make_async_copy(mask, valid, in_sem.at[1]),
        pltpu.make_async_copy(basis, mix, in_sem.at[2]),
    ]
    for load in small:
        load.start()

    for load in words:
        load.wait()
    for layer in range(LOCAL):
        table(layer, shift, frac, band, corner)

    def compute(first, count):
        for i in range(first, first + count):
            loads[i].wait()

        def lanes(low):
            return jnp.concatenate(
                [
                    volbuf[first : first + count, layer, :, low : low + BLOCK].reshape(count * BLOCK, BLOCK)
                    for layer in range(LOCAL)
                ],
                axis=1,
            )

        for q, piece in enumerate(banded(lanes, band[...], corner[...])):
            part[first : first + count, :, :, :, :, q * HALF : (q + 1) * HALF] = piece.reshape(
                count, 2, COEF, 2, COEF, HALF
            )

    shares = [remote(part.at[i, 1 - core], theirs.at[i], pair_send.at[i], pair_recv.at[i]) for i in range(8)]

    def is_self(i, dyl, dx):
        return ORDER[i] == (0, 0) and dyl == 0 and dx == 0

    def dispatch(r, i):
        dz, dyh = ORDER[i]
        if r == 0:
            shares[i].wait_recv()
        outgoing[r, i] = (part[i, core, :, r] + theirs[i, :, r]).astype(jnp.bfloat16)
        for dyl in range(2):
            for dx in range(4):
                tyl, tx = yl ^ dyl, (x + dx) % 4
                source = outgoing.at[r, i, tyl * 4 + tx]
                target = incoming.at[r, i, mine]
                if is_self(i, dyl, dx):
                    pltpu.make_async_copy(source, target, self_sem.at[r]).start()
                else:
                    to = device(tx, tyl, yh ^ dyh, (z + dz) % 4, core)
                    remote(source, target, send_sem.at[r, i], recv_sem.at[r, i], to).start()

    done, ready = 0, 0
    for first, count in GROUPS:
        compute(first, count)
        if first == 0:
            pl.semaphore_wait(barrier, 64)
        for i in range(first, first + count):
            shares[i].start()
        while done < ready:
            dispatch(0, done)
            done += 1
        ready = first + count
    while done < 8:
        dispatch(0, done)
        done += 1
    for i in range(8):
        dispatch(1, i)

    for pair in range(LOCAL // 2):
        back[pair] = back_table(shift, frac, pair)
    store_tables = pltpu.make_async_copy(back, tables, in_sem.at[3])
    store_tables.start()
    for load in small:
        load.wait()
    turned = mix[...].astype(jnp.float32).T.astype(jnp.bfloat16)

    for r in range(2):
        for i in range(8):
            count = 8
            if ORDER[i] == (0, 0):
                pltpu.make_async_copy(outgoing.at[r, i, 0], incoming.at[r, i, 0], self_sem.at[r]).wait()
                count = 7
            remote(
                outgoing.at[r, i, pl.ds(0, count)], incoming.at[r, i, pl.ds(0, count)],
                send_sem.at[r, i], recv_sem.at[r, i],
            ).wait_recv()
            piece = incoming[r, i].astype(jnp.float32).reshape(64, X)
            if i == 0:
                total[r] = piece
            else:
                total[r] += piece
        proj = total[r]
        high = proj.astype(jnp.bfloat16)
        low = (proj - high.astype(jnp.float32)).astype(jnp.bfloat16)
        predicted = jnp.dot(turned, high, preferred_element_type=jnp.float32) + jnp.dot(
            turned, low, preferred_element_type=jnp.float32
        )
        residual = (valid[r].astype(jnp.float32) * (predicted - jnp.sqrt(wanted[r]))).astype(jnp.bfloat16)
        res_buf[r] = residual
        slab = 2.0 * jnp.dot(mix[...], residual, preferred_element_type=jnp.float32)
        gp[r] = slab.reshape(COEF, COEF, X).astype(jnp.bfloat16)
        for i, (dz, dyh) in enumerate(ORDER):
            for dyl in range(2):
                for dx in range(4):
                    tyl, tx = yl ^ dyl, (x + dx) % 4
                    source = gp.at[r, tyl * 4 + tx]
                    target = gathered.at[z * 2 + yh, mine, r]
                    if is_self(i, dyl, dx):
                        pltpu.make_async_copy(source, target, self_sem.at[r]).start()
                    else:
                        to = device(tx, tyl, yh ^ dyh, (z + dz) % 4, core)
                        remote(source, target, back_send.at[r, i], back_recv.at[r, i], to).start()

    store_res = pltpu.make_async_copy(res_buf, resid, in_sem.at[0])
    store_res.start()
    store_tables.wait()
    for i in range(8):
        shares[i].wait_send()
        for r in range(2):
            remote(
                outgoing.at[r, i, pl.ds(0, KEPT[i])], incoming.at[r, i, pl.ds(0, KEPT[i])],
                send_sem.at[r, i], recv_sem.at[r, i],
            ).wait_send()
    passes = []
    for r in range(2):
        if r == 1:
            for i in range(8):
                remote(
                    gp.at[0, pl.ds(0, KEPT[i])], incoming.at[0, i, pl.ds(0, KEPT[i])],
                    back_send.at[0, i], back_recv.at[0, i],
                ).wait_send()
            for store in passes:
                store.wait()
            passes = []
        for i, (dz, dyh) in enumerate(ORDER):
            block = ((z + 4 - dz) % 4) * 2 + (yh ^ dyh)
            rows = gathered.at[block, :, r]
            count = 8
            if ORDER[i] == (0, 0):
                pltpu.make_async_copy(gp.at[r, 0], gathered.at[block, 0, r], self_sem.at[r]).wait()
                count = 7
            remote(
                gp.at[r, pl.ds(0, count)], gathered.at[block, pl.ds(0, count), r],
                back_send.at[r, i], back_recv.at[r, i],
            ).wait_recv()
            home = grad_rows.at[block, core, :, r]
            onward = remote(rows, home, share_send.at[r, i], share_recv.at[r, i])
            onward.start()
            store = pltpu.make_async_copy(rows, home, out_sem.at[r, i])
            store.start()
            passes += [onward, store]
    for store in passes + [store_res]:
        store.wait()
    for i in range(8):
        remote(
            gp.at[1, pl.ds(0, KEPT[i])], incoming.at[1, i, pl.ds(0, KEPT[i])], back_send.at[1, i], back_recv.at[1, i]
        ).wait_send()


def back_project(
    rows_hbm, tables_hbm, res_in, shift_hbm, grad, res_out,
    rows_ref, tables, res_buf, shift, staged, load_sem, small_sem, sem,
):
    size = rows_ref.shape[1]
    words = pltpu.make_async_copy(shift_hbm, shift, small_sem.at[1])
    load_tables = pltpu.make_async_copy(tables_hbm, tables, small_sem.at[0])
    loads = [
        pltpu.make_async_copy(rows_hbm.at[pl.ds(t * size, size)], rows_ref.at[t], load_sem.at[t]) for t in range(PIECES)
    ]
    last = pltpu.make_async_copy(res_in, res_buf, small_sem.at[2])
    for load in [load_tables, loads[0], words] + loads[1:] + [last]:
        load.start()
    load_tables.wait()
    stores = []
    for t in range(PIECES):
        loads[t].wait()
        empty = jnp.zeros((size, HALF), jnp.bfloat16)
        windows = [jnp.concatenate([empty, rows_ref[t, :, :HALF]], axis=1)]
        windows += [rows_ref[t, :, q * HALF : q * HALF + BLOCK] for q in range(3)]
        windows += [jnp.concatenate([rows_ref[t, :, 3 * HALF :], empty], axis=1)]
        if t == 0:
            words.wait()
        for pair in range(LOCAL // 2):
            for n, window in enumerate(windows):
                wide = jnp.dot(window, tables[pair], preferred_element_type=jnp.float32).astype(jnp.bfloat16)
                for half in range(2):
                    staged[t, 2 * pair + half, :, n * HALF : (n + 1) * HALF] = wide[:, half * HALF : (half + 1) * HALF]
            for layer in (2 * pair, 2 * pair + 1):
                first = pl.multiple_of(jnp.where(shift[layer] < 0, 0, HALF), HALF)
                store = pltpu.make_async_copy(
                    staged.at[t, layer, :, pl.ds(first, X)],
                    grad.at[layer, pl.ds(t * size, size)],
                    sem.at[t * LOCAL + layer],
                )
                store.start()
                stores.append(store)
        if t == 0:
            last.wait()
            keep = pltpu.make_async_copy(res_buf, res_out, small_sem.at[0])
            keep.start()
            stores.append(keep)
    for store in stores:
        store.wait()


def shards(volume, shift, frac, basis, data, mask):
    layers, rows, coefs, cols = volume.shape
    flat = rows * coefs
    hbm = pl.BlockSpec(memory_space=pl.ANY)
    dma = pltpu.SemaphoreType.DMA
    tall = layers * BLOCK
    grad_rows, tables, resid = pl.pallas_call(
        exchange,
        out_shape=(
            jax.ShapeDtypeStruct((8, 2, 8, 2, coefs, cols), jnp.bfloat16),
            jax.ShapeDtypeStruct((layers // 2, BLOCK, BLOCK), jnp.bfloat16),
            jax.ShapeDtypeStruct(data.shape, jnp.bfloat16),
        ),
        in_specs=[hbm] * 6,
        out_specs=(hbm, hbm, hbm),
        scratch_shapes=[
            pltpu.VMEM((8, layers, BLOCK, cols), jnp.bfloat16),
            pltpu.SMEM(shift.shape, jnp.int32),
            pltpu.SMEM(frac.shape, jnp.int32),
            pltpu.VMEM((tall, BLOCK), jnp.bfloat16),
            pltpu.VMEM((tall, BLOCK), jnp.bfloat16),
            pltpu.VMEM((layers // 2, BLOCK, BLOCK), jnp.bfloat16),
            pltpu.VMEM((8, 8, 2, coefs, cols), jnp.bfloat16),
            pltpu.VMEM(data.shape, jnp.bfloat16),
            pltpu.VMEM((8, 2, 8, 2, coefs, cols), jnp.float32),
            pltpu.VMEM((8, 8, 2, coefs, cols), jnp.float32),
            pltpu.VMEM((2, 8, 8, coefs, cols), jnp.bfloat16),
            pltpu.VMEM((2, 8, 8, coefs, cols), jnp.bfloat16),
            pltpu.VMEM((2, 64, cols), jnp.float32),
            pltpu.VMEM(data.shape, jnp.float32),
            pltpu.VMEM(mask.shape, jnp.int32),
            pltpu.VMEM(basis.shape, jnp.bfloat16),
            pltpu.VMEM((2, 8, coefs, cols), jnp.bfloat16),
            dma((8,)), dma((5,)), dma((2,)), dma((8,)), dma((8,)), dma((2, 8)), dma((2, 8)),
            dma((2, 8)), dma((2, 8)), dma((2, 8)), dma((2, 8)), dma((2, 8)),
        ],
        compiler_params=pltpu.CompilerParams(collective_id=0, has_side_effects=True, vmem_limit_bytes=VMEM),
        name="exchange",
    )(volume.reshape(layers, flat, cols), shift, frac, basis, data, mask)
    gradient, residual = pl.pallas_call(
        back_project,
        out_shape=(
            jax.ShapeDtypeStruct((layers, flat, cols), jnp.bfloat16),
            jax.ShapeDtypeStruct(data.shape, jnp.bfloat16),
        ),
        in_specs=[hbm] * 4,
        out_specs=(hbm, hbm),
        scratch_shapes=[
            pltpu.VMEM((PIECES, flat // PIECES, cols), jnp.bfloat16),
            pltpu.VMEM((layers // 2, BLOCK, BLOCK), jnp.bfloat16),
            pltpu.VMEM(data.shape, jnp.bfloat16),
            pltpu.SMEM(shift.shape, jnp.int32),
            pltpu.VMEM((PIECES, layers, flat // PIECES, cols + HALF), jnp.bfloat16),
            dma((PIECES,)),
            dma((3,)),
            dma((PIECES * layers,)),
        ],
        compiler_params=pltpu.CompilerParams(vmem_limit_bytes=VMEM),
        name="back_project",
    )(grad_rows.reshape(flat, cols), tables, resid, shift)
    return gradient.reshape(volume.shape), residual


def solution(mesh):
    in_specs = (
        P("depth", None, "coef", None),
        P("depth"),
        P("depth"),
        P(),
        P(("depth", "coef"), None, None),
        P(("depth", "coef"), None, None),
    )
    out_specs = (P("depth", None, "coef", None), P(("depth", "coef"), None, None))
    return jax.shard_map(shards, mesh=mesh, in_specs=in_specs, out_specs=out_specs, check_vma=False)
```

```python
import functools

import jax
import jax.numpy as jnp
from jax import lax
from jax.experimental import pallas as pl
from jax.experimental.pallas import tpu as pltpu
from jax.sharding import PartitionSpec as P

MESH = pl.DeviceIdType.MESH
X = 512
LOCAL = 4
COEF = 8
BLOCK = 256
HALF = 128
PEERS = sorted(
    ((dz, dyh, dyl, dx) for dz in range(4) for dyh in range(2) for dyl in range(2) for dx in range(4)),
    key=lambda p: min(p[0], 4 - p[0]) + (1 if p[2] else 2 * p[1]) + min(p[3], 4 - p[3]),
)[:0:-1]
GROUPS = ((0, 4), (4, 2), (6, 2))
VMEM = 60 * 1024 * 1024
PIECES = ((0, 512), (512, 1024), (1536, 512))
ORDER = ((1, 0), (0, 1), (2, 0), (3, 1), (1, 1), (2, 1), (3, 0), (0, 0))
KEPT = tuple(7 if pair == (0, 0) else 8 for pair in ORDER)


def place():
    d = lax.axis_index("depth")
    c = lax.axis_index("coef")
    return c % 4, c // 4, (d // 2) % 2, d // 4, d % 2


def device(x, yl, yh, z, core):
    return {"depth": z * 4 + yh * 2 + core, "coef": yl * 4 + x}


def table(layer, shift, frac, band, corner):
    s = shift[layer]
    w = frac[layer].astype(jnp.float32) * 0.0625
    rows = lax.broadcasted_iota(jnp.int32, (BLOCK, BLOCK), 0)
    cols = lax.broadcasted_iota(jnp.int32, (BLOCK, BLOCK), 1)
    gap = cols - rows - s
    tile = jnp.where(gap == 0, 1.0 - w, jnp.where(gap == 1, w, 0.0)).astype(jnp.bfloat16)
    empty = jnp.zeros((HALF, HALF), jnp.bfloat16)
    span = pl.ds(layer * BLOCK, BLOCK)
    band[span] = tile
    corner[span] = jnp.concatenate(
        [
            jnp.concatenate([empty, tile[:HALF, HALF:]], axis=1),
            jnp.concatenate([tile[HALF:, :HALF], empty], axis=1),
        ],
        axis=0,
    )


def back_table(shift, frac, pair):
    rows = lax.broadcasted_iota(jnp.int32, (BLOCK, HALF), 0)
    cols = lax.broadcasted_iota(jnp.int32, (BLOCK, HALF), 1)
    halves = []
    for layer in (2 * pair, 2 * pair + 1):
        s = shift[layer]
        w = frac[layer].astype(jnp.float32) * 0.0625
        gap = rows - cols - jnp.where(s < 0, s + HALF, s)
        halves.append(jnp.where(gap == 0, 1.0 - w, jnp.where(gap == 1, w, 0.0)).astype(jnp.bfloat16))
    return jnp.concatenate(halves, axis=1)


def banded(lanes, band, corner):
    low, middle, high = lanes(0), lanes(HALF), lanes(BLOCK)
    m = low.shape[0]
    sides = jnp.dot(jnp.concatenate([low, high], axis=0), band, preferred_element_type=jnp.float32)
    inner = jnp.dot(middle, corner, preferred_element_type=jnp.float32)
    return (
        sides[:m, :HALF],
        sides[:m, HALF:] + inner[:, :HALF],
        sides[m:, :HALF] + inner[:, HALF:],
        sides[m:, HALF:],
    )


def exchange(
    vol, shift_hbm, frac_hbm, basis, data, mask,
    grad_rows, tables, resid,
    volbuf, shift, frac, band, corner, back, gathered, res_buf, part, theirs, outgoing, incoming, total, wanted, valid, mix, gp,
    vol_sem, in_sem, self_sem, pair_send, pair_recv, send_sem, recv_sem, back_send, back_recv,
    share_send, share_recv, out_sem,
):
    x, yl, yh, z, core = place()
    mine = yl * 4 + x
    partner = device(x, yl, yh, z, 1 - core)

    def remote(source, target, send, recv, to=partner):
        return pltpu.make_async_remote_copy(source, target, send, recv, device_id=to, device_id_type=MESH)

    words = [
        pltpu.make_async_copy(shift_hbm, shift, in_sem.at[3]),
        pltpu.make_async_copy(frac_hbm, frac, in_sem.at[4]),
    ]
    for load in words:
        load.start()
    loads = []
    for i, (dz, dyh) in enumerate(ORDER):
        block = ((z + dz) % 4) * 2 + (yh ^ dyh)
        load = pltpu.make_async_copy(
            vol.at[:, pl.ds(pl.multiple_of(block * BLOCK, BLOCK), BLOCK)], volbuf.at[i], vol_sem.at[i]
        )
        load.start()
        loads.append(load)
    barrier = pltpu.get_barrier_semaphore()
    for dz, dyh, dyl, dx in PEERS:
        to = device((x + dx) % 4, yl ^ dyl, yh ^ dyh, (z + dz) % 4, core)
        pl.semaphore_signal(barrier, inc=1, device_id=to, device_id_type=MESH)
    pl.semaphore_signal(barrier, inc=1, device_id=partner, device_id_type=MESH)

    small = [
        pltpu.make_async_copy(data, wanted, in_sem.at[0]),
        pltpu.make_async_copy(mask, valid, in_sem.at[1]),
        pltpu.make_async_copy(basis, mix, in_sem.at[2]),
    ]
    for load in small:
        load.start()

    for load in words:
        load.wait()
    for layer in range(LOCAL):
        table(layer, shift, frac, band, corner)

    def compute(first, count):
        for i in range(first, first + count):
            loads[i].wait()

        def lanes(low):
            return jnp.concatenate(
                [
                    volbuf[first : first + count, layer, :, low : low + BLOCK].reshape(count * BLOCK, BLOCK)
                    for layer in range(LOCAL)
                ],
                axis=1,
            )

        for q, piece in enumerate(banded(lanes, band[...], corner[...])):
            part[first : first + count, :, :, :, :, q * HALF : (q + 1) * HALF] = piece.reshape(
                count, 2, COEF, 2, COEF, HALF
            )

    shares = [remote(part.at[i, 1 - core], theirs.at[i], pair_send.at[i], pair_recv.at[i]) for i in range(8)]

    def is_self(i, dyl, dx):
        return ORDER[i] == (0, 0) and dyl == 0 and dx == 0

    def dispatch(r, i):
        dz, dyh = ORDER[i]
        if r == 0:
            shares[i].wait_recv()
        outgoing[r, i] = (part[i, core, :, r] + theirs[i, :, r]).astype(jnp.bfloat16)
        for dyl in range(2):
            for dx in range(4):
                tyl, tx = yl ^ dyl, (x + dx) % 4
                source = outgoing.at[r, i, tyl * 4 + tx]
                target = incoming.at[r, i, mine]
                if is_self(i, dyl, dx):
                    pltpu.make_async_copy(source, target, self_sem.at[r]).start()
                else:
                    to = device(tx, tyl, yh ^ dyh, (z + dz) % 4, core)
                    remote(source, target, send_sem.at[r, i], recv_sem.at[r, i], to).start()

    done, ready = 0, 0
    for first, count in GROUPS:
        compute(first, count)
        if first == 0:
            pl.semaphore_wait(barrier, 64)
        for i in range(first, first + count):
            shares[i].start()
        while done < ready:
            dispatch(0, done)
            done += 1
        ready = first + count
    while done < 8:
        dispatch(0, done)
        done += 1
    for i in range(8):
        dispatch(1, i)

    for pair in range(LOCAL // 2):
        back[pair] = back_table(shift, frac, pair)
    store_tables = pltpu.make_async_copy(back, tables, in_sem.at[3])
    store_tables.start()
    for load in small:
        load.wait()
    turned = mix[...].astype(jnp.float32).T.astype(jnp.bfloat16)

    for r in range(2):
        for i in range(8):
            count = 8
            if ORDER[i] == (0, 0):
                pltpu.make_async_copy(outgoing.at[r, i, 0], incoming.at[r, i, 0], self_sem.at[r]).wait()
                count = 7
            remote(
                outgoing.at[r, i, pl.ds(0, count)], incoming.at[r, i, pl.ds(0, count)],
                send_sem.at[r, i], recv_sem.at[r, i],
            ).wait_recv()
            piece = incoming[r, i].astype(jnp.float32).reshape(64, X)
            if i == 0:
                total[r] = piece
            else:
                total[r] += piece
        proj = total[r]
        high = proj.astype(jnp.bfloat16)
        low = (proj - high.astype(jnp.float32)).astype(jnp.bfloat16)
        predicted = jnp.dot(turned, high, preferred_element_type=jnp.float32) + jnp.dot(
            turned, low, preferred_element_type=jnp.float32
        )
        residual = (valid[r].astype(jnp.float32) * (predicted - jnp.sqrt(wanted[r]))).astype(jnp.bfloat16)
        res_buf[r] = residual
        slab = 2.0 * jnp.dot(mix[...], residual, preferred_element_type=jnp.float32)
        gp[r] = slab.reshape(COEF, COEF, X).astype(jnp.bfloat16)
        for i, (dz, dyh) in enumerate(ORDER):
            for dyl in range(2):
                for dx in range(4):
                    tyl, tx = yl ^ dyl, (x + dx) % 4
                    source = gp.at[r, tyl * 4 + tx]
                    target = gathered.at[z * 2 + yh, mine, r]
                    if is_self(i, dyl, dx):
                        pltpu.make_async_copy(source, target, self_sem.at[r]).start()
                    else:
                        to = device(tx, tyl, yh ^ dyh, (z + dz) % 4, core)
                        remote(source, target, back_send.at[r, i], back_recv.at[r, i], to).start()

    store_res = pltpu.make_async_copy(res_buf, resid, in_sem.at[0])
    store_res.start()
    store_tables.wait()
    for i in range(8):
        shares[i].wait_send()
        for r in range(2):
            remote(
                outgoing.at[r, i, pl.ds(0, KEPT[i])], incoming.at[r, i, pl.ds(0, KEPT[i])],
                send_sem.at[r, i], recv_sem.at[r, i],
            ).wait_send()
    passes = []
    for r in range(2):
        if r == 1:
            for i in range(8):
                remote(
                    gp.at[0, pl.ds(0, KEPT[i])], incoming.at[0, i, pl.ds(0, KEPT[i])],
                    back_send.at[0, i], back_recv.at[0, i],
                ).wait_send()
            for store in passes:
                store.wait()
            passes = []
        for i, (dz, dyh) in enumerate(ORDER):
            block = ((z + 4 - dz) % 4) * 2 + (yh ^ dyh)
            rows = gathered.at[block, :, r]
            count = 8
            if ORDER[i] == (0, 0):
                pltpu.make_async_copy(gp.at[r, 0], gathered.at[block, 0, r], self_sem.at[r]).wait()
                count = 7
            remote(
                gp.at[r, pl.ds(0, count)], gathered.at[block, pl.ds(0, count), r],
                back_send.at[r, i], back_recv.at[r, i],
            ).wait_recv()
            home = grad_rows.at[block, core, :, r]
            onward = remote(rows, home, share_send.at[r, i], share_recv.at[r, i])
            onward.start()
            store = pltpu.make_async_copy(rows, home, out_sem.at[r, i])
            store.start()
            passes += [onward, store]
    for store in passes + [store_res]:
        store.wait()
    for i in range(8):
        remote(
            gp.at[1, pl.ds(0, KEPT[i])], incoming.at[1, i, pl.ds(0, KEPT[i])], back_send.at[1, i], back_recv.at[1, i]
        ).wait_send()


def back_project(
    rows_hbm, tables_hbm, res_in, shift_hbm, grad, res_out,
    rows_ref, tables, res_buf, shift, staged, load_sem, small_sem, sem,
):
    words = pltpu.make_async_copy(shift_hbm, shift, small_sem.at[1])
    load_tables = pltpu.make_async_copy(tables_hbm, tables, small_sem.at[0])
    loads = [
        pltpu.make_async_copy(rows_hbm.at[pl.ds(low, size)], rows_ref.at[pl.ds(low, size)], load_sem.at[t])
        for t, (low, size) in enumerate(PIECES)
    ]
    last = pltpu.make_async_copy(res_in, res_buf, small_sem.at[2])
    for load in [load_tables, loads[0], words] + loads[1:] + [last]:
        load.start()
    load_tables.wait()
    stores = []
    for t, (low, size) in enumerate(PIECES):
        span = pl.ds(low, size)
        loads[t].wait()
        empty = jnp.zeros((size, HALF), jnp.bfloat16)
        windows = [jnp.concatenate([empty, rows_ref[span, :HALF]], axis=1)]
        windows += [rows_ref[span, q * HALF : q * HALF + BLOCK] for q in range(3)]
        windows += [jnp.concatenate([rows_ref[span, 3 * HALF :], empty], axis=1)]
        if t == 0:
            words.wait()
        for pair in range(LOCAL // 2):
            for n, window in enumerate(windows):
                wide = jnp.dot(window, tables[pair], preferred_element_type=jnp.float32).astype(jnp.bfloat16)
                for half in range(2):
                    staged[2 * pair + half, span, n * HALF : (n + 1) * HALF] = wide[:, half * HALF : (half + 1) * HALF]
            for layer in (2 * pair, 2 * pair + 1):
                first = pl.multiple_of(jnp.where(shift[layer] < 0, 0, HALF), HALF)
                store = pltpu.make_async_copy(
                    staged.at[layer, span, pl.ds(first, X)],
                    grad.at[layer, span],
                    sem.at[t * LOCAL + layer],
                )
                store.start()
                stores.append(store)
        if t == 0:
            last.wait()
            keep = pltpu.make_async_copy(res_buf, res_out, small_sem.at[0])
            keep.start()
            stores.append(keep)
    for store in stores:
        store.wait()


def shards(volume, shift, frac, basis, data, mask):
    layers, rows, coefs, cols = volume.shape
    flat = rows * coefs
    hbm = pl.BlockSpec(memory_space=pl.ANY)
    dma = pltpu.SemaphoreType.DMA
    tall = layers * BLOCK
    grad_rows, tables, resid = pl.pallas_call(
        exchange,
        out_shape=(
            jax.ShapeDtypeStruct((8, 2, 8, 2, coefs, cols), jnp.bfloat16),
            jax.ShapeDtypeStruct((layers // 2, BLOCK, BLOCK), jnp.bfloat16),
            jax.ShapeDtypeStruct(data.shape, jnp.bfloat16),
        ),
        in_specs=[hbm] * 6,
        out_specs=(hbm, hbm, hbm),
        scratch_shapes=[
            pltpu.VMEM((8, layers, BLOCK, cols), jnp.bfloat16),
            pltpu.SMEM(shift.shape, jnp.int32),
            pltpu.SMEM(frac.shape, jnp.int32),
            pltpu.VMEM((tall, BLOCK), jnp.bfloat16),
            pltpu.VMEM((tall, BLOCK), jnp.bfloat16),
            pltpu.VMEM((layers // 2, BLOCK, BLOCK), jnp.bfloat16),
            pltpu.VMEM((8, 8, 2, coefs, cols), jnp.bfloat16),
            pltpu.VMEM(data.shape, jnp.bfloat16),
            pltpu.VMEM((8, 2, 8, 2, coefs, cols), jnp.float32),
            pltpu.VMEM((8, 8, 2, coefs, cols), jnp.float32),
            pltpu.VMEM((2, 8, 8, coefs, cols), jnp.bfloat16),
            pltpu.VMEM((2, 8, 8, coefs, cols), jnp.bfloat16),
            pltpu.VMEM((2, 64, cols), jnp.float32),
            pltpu.VMEM(data.shape, jnp.float32),
            pltpu.VMEM(mask.shape, jnp.int32),
            pltpu.VMEM(basis.shape, jnp.bfloat16),
            pltpu.VMEM((2, 8, coefs, cols), jnp.bfloat16),
            dma((8,)), dma((5,)), dma((2,)), dma((8,)), dma((8,)), dma((2, 8)), dma((2, 8)),
            dma((2, 8)), dma((2, 8)), dma((2, 8)), dma((2, 8)), dma((2, 8)),
        ],
        compiler_params=pltpu.CompilerParams(collective_id=0, has_side_effects=True, vmem_limit_bytes=VMEM),
        name="exchange",
    )(volume.reshape(layers, flat, cols), shift, frac, basis, data, mask)
    gradient, residual = pl.pallas_call(
        back_project,
        out_shape=(
            jax.ShapeDtypeStruct((layers, flat, cols), jnp.bfloat16),
            jax.ShapeDtypeStruct(data.shape, jnp.bfloat16),
        ),
        in_specs=[hbm] * 4,
        out_specs=(hbm, hbm),
        scratch_shapes=[
            pltpu.VMEM((flat, cols), jnp.bfloat16),
            pltpu.VMEM((layers // 2, BLOCK, BLOCK), jnp.bfloat16),
            pltpu.VMEM(data.shape, jnp.bfloat16),
            pltpu.SMEM(shift.shape, jnp.int32),
            pltpu.VMEM((layers, flat, cols + HALF), jnp.bfloat16),
            dma((len(PIECES),)),
            dma((3,)),
            dma((len(PIECES) * layers,)),
        ],
        compiler_params=pltpu.CompilerParams(vmem_limit_bytes=VMEM),
        name="back_project",
    )(grad_rows.reshape(flat, cols), tables, resid, shift)
    return gradient.reshape(volume.shape), residual


def solution(mesh):
    in_specs = (
        P("depth", None, "coef", None),
        P("depth"),
        P("depth"),
        P(),
        P(("depth", "coef"), None, None),
        P(("depth", "coef"), None, None),
    )
    out_specs = (P("depth", None, "coef", None), P(("depth", "coef"), None, None))
    return jax.shard_map(shards, mesh=mesh, in_specs=in_specs, out_specs=out_specs, check_vma=False)
```

```python
import functools

import jax
import jax.numpy as jnp
from jax import lax
from jax.experimental import pallas as pl
from jax.experimental.pallas import tpu as pltpu
from jax.sharding import PartitionSpec as P

MESH = pl.DeviceIdType.MESH
X = 512
LOCAL = 4
COEF = 8
BLOCK = 256
HALF = 128
PEERS = sorted(
    ((dz, dyh, dyl, dx) for dz in range(4) for dyh in range(2) for dyl in range(2) for dx in range(4)),
    key=lambda p: min(p[0], 4 - p[0]) + (1 if p[2] else 2 * p[1]) + min(p[3], 4 - p[3]),
)[:0:-1]
GROUPS = ((0, 4), (4, 2), (6, 2))
VMEM = 60 * 1024 * 1024
PIECES = ((0, 512), (512, 1280), (1792, 256))
ORDER = ((1, 0), (0, 1), (2, 0), (3, 1), (1, 1), (2, 1), (3, 0), (0, 0))
KEPT = tuple(7 if pair == (0, 0) else 8 for pair in ORDER)


def place():
    d = lax.axis_index("depth")
    c = lax.axis_index("coef")
    return c % 4, c // 4, (d // 2) % 2, d // 4, d % 2


def device(x, yl, yh, z, core):
    return {"depth": z * 4 + yh * 2 + core, "coef": yl * 4 + x}


def table(layer, shift, frac, band, corner):
    s = shift[layer]
    w = frac[layer].astype(jnp.float32) * 0.0625
    rows = lax.broadcasted_iota(jnp.int32, (BLOCK, BLOCK), 0)
    cols = lax.broadcasted_iota(jnp.int32, (BLOCK, BLOCK), 1)
    gap = cols - rows - s
    tile = jnp.where(gap == 0, 1.0 - w, jnp.where(gap == 1, w, 0.0)).astype(jnp.bfloat16)
    empty = jnp.zeros((HALF, HALF), jnp.bfloat16)
    span = pl.ds(layer * BLOCK, BLOCK)
    band[span] = tile
    corner[span] = jnp.concatenate(
        [
            jnp.concatenate([empty, tile[:HALF, HALF:]], axis=1),
            jnp.concatenate([tile[HALF:, :HALF], empty], axis=1),
        ],
        axis=0,
    )


def back_table(shift, frac, pair):
    rows = lax.broadcasted_iota(jnp.int32, (BLOCK, HALF), 0)
    cols = lax.broadcasted_iota(jnp.int32, (BLOCK, HALF), 1)
    halves = []
    for layer in (2 * pair, 2 * pair + 1):
        s = shift[layer]
        w = frac[layer].astype(jnp.float32) * 0.0625
        gap = rows - cols - jnp.where(s < 0, s + HALF, s)
        halves.append(jnp.where(gap == 0, 1.0 - w, jnp.where(gap == 1, w, 0.0)).astype(jnp.bfloat16))
    return jnp.concatenate(halves, axis=1)


def banded(lanes, band, corner):
    low, middle, high = lanes(0), lanes(HALF), lanes(BLOCK)
    m = low.shape[0]
    sides = jnp.dot(jnp.concatenate([low, high], axis=0), band, preferred_element_type=jnp.float32)
    inner = jnp.dot(middle, corner, preferred_element_type=jnp.float32)
    return (
        sides[:m, :HALF],
        sides[:m, HALF:] + inner[:, :HALF],
        sides[m:, :HALF] + inner[:, HALF:],
        sides[m:, HALF:],
    )


def exchange(
    vol, shift_hbm, frac_hbm, basis, data, mask,
    grad_rows, tables, resid,
    volbuf, shift, frac, band, corner, back, gathered, res_buf, part, theirs, outgoing, incoming, total, wanted, valid, mix, gp,
    vol_sem, in_sem, self_sem, pair_send, pair_recv, send_sem, recv_sem, back_send, back_recv,
    share_send, share_recv, out_sem,
):
    x, yl, yh, z, core = place()
    mine = yl * 4 + x
    partner = device(x, yl, yh, z, 1 - core)

    def remote(source, target, send, recv, to=partner):
        return pltpu.make_async_remote_copy(source, target, send, recv, device_id=to, device_id_type=MESH)

    words = [
        pltpu.make_async_copy(shift_hbm, shift, in_sem.at[3]),
        pltpu.make_async_copy(frac_hbm, frac, in_sem.at[4]),
    ]
    for load in words:
        load.start()
    loads = []
    for i, (dz, dyh) in enumerate(ORDER):
        block = ((z + dz) % 4) * 2 + (yh ^ dyh)
        load = pltpu.make_async_copy(
            vol.at[:, pl.ds(pl.multiple_of(block * BLOCK, BLOCK), BLOCK)], volbuf.at[i], vol_sem.at[i]
        )
        load.start()
        loads.append(load)
    barrier = pltpu.get_barrier_semaphore()
    for dz, dyh, dyl, dx in PEERS:
        to = device((x + dx) % 4, yl ^ dyl, yh ^ dyh, (z + dz) % 4, core)
        pl.semaphore_signal(barrier, inc=1, device_id=to, device_id_type=MESH)
    pl.semaphore_signal(barrier, inc=1, device_id=partner, device_id_type=MESH)

    small = [
        pltpu.make_async_copy(data, wanted, in_sem.at[0]),
        pltpu.make_async_copy(mask, valid, in_sem.at[1]),
        pltpu.make_async_copy(basis, mix, in_sem.at[2]),
    ]
    for load in small:
        load.start()

    for load in words:
        load.wait()
    for layer in range(LOCAL):
        table(layer, shift, frac, band, corner)

    def compute(first, count):
        for i in range(first, first + count):
            loads[i].wait()

        def lanes(low):
            return jnp.concatenate(
                [
                    volbuf[first : first + count, layer, :, low : low + BLOCK].reshape(count * BLOCK, BLOCK)
                    for layer in range(LOCAL)
                ],
                axis=1,
            )

        for q, piece in enumerate(banded(lanes, band[...], corner[...])):
            part[first : first + count, :, :, :, :, q * HALF : (q + 1) * HALF] = piece.reshape(
                count, 2, COEF, 2, COEF, HALF
            )

    shares = [remote(part.at[i, 1 - core], theirs.at[i], pair_send.at[i], pair_recv.at[i]) for i in range(8)]

    def is_self(i, dyl, dx):
        return ORDER[i] == (0, 0) and dyl == 0 and dx == 0

    def dispatch(r, i):
        dz, dyh = ORDER[i]
        if r == 0:
            shares[i].wait_recv()
        outgoing[r, i] = (part[i, core, :, r] + theirs[i, :, r]).astype(jnp.bfloat16)
        for dyl in range(2):
            for dx in range(4):
                tyl, tx = yl ^ dyl, (x + dx) % 4
                source = outgoing.at[r, i, tyl * 4 + tx]
                target = incoming.at[r, i, mine]
                if is_self(i, dyl, dx):
                    pltpu.make_async_copy(source, target, self_sem.at[r]).start()
                else:
                    to = device(tx, tyl, yh ^ dyh, (z + dz) % 4, core)
                    remote(source, target, send_sem.at[r, i], recv_sem.at[r, i], to).start()

    done, ready = 0, 0
    for first, count in GROUPS:
        compute(first, count)
        if first == 0:
            pl.semaphore_wait(barrier, 64)
        for i in range(first, first + count):
            shares[i].start()
        while done < ready:
            dispatch(0, done)
            done += 1
        ready = first + count
    while done < 8:
        dispatch(0, done)
        done += 1
    for i in range(8):
        dispatch(1, i)

    for pair in range(LOCAL // 2):
        back[pair] = back_table(shift, frac, pair)
    store_tables = pltpu.make_async_copy(back, tables, in_sem.at[3])
    store_tables.start()
    for load in small:
        load.wait()
    turned = mix[...].astype(jnp.float32).T.astype(jnp.bfloat16)

    for r in range(2):
        for i in range(8):
            count = 8
            if ORDER[i] == (0, 0):
                pltpu.make_async_copy(outgoing.at[r, i, 0], incoming.at[r, i, 0], self_sem.at[r]).wait()
                count = 7
            remote(
                outgoing.at[r, i, pl.ds(0, count)], incoming.at[r, i, pl.ds(0, count)],
                send_sem.at[r, i], recv_sem.at[r, i],
            ).wait_recv()
            piece = incoming[r, i].astype(jnp.float32).reshape(64, X)
            if i == 0:
                total[r] = piece
            else:
                total[r] += piece
        proj = total[r]
        high = proj.astype(jnp.bfloat16)
        low = (proj - high.astype(jnp.float32)).astype(jnp.bfloat16)
        predicted = jnp.dot(turned, high, preferred_element_type=jnp.float32) + jnp.dot(
            turned, low, preferred_element_type=jnp.float32
        )
        residual = (valid[r].astype(jnp.float32) * (predicted - jnp.sqrt(wanted[r]))).astype(jnp.bfloat16)
        res_buf[r] = residual
        slab = 2.0 * jnp.dot(mix[...], residual, preferred_element_type=jnp.float32)
        gp[r] = slab.reshape(COEF, COEF, X).astype(jnp.bfloat16)
        for i, (dz, dyh) in enumerate(ORDER):
            for dyl in range(2):
                for dx in range(4):
                    tyl, tx = yl ^ dyl, (x + dx) % 4
                    source = gp.at[r, tyl * 4 + tx]
                    target = gathered.at[z * 2 + yh, mine, r]
                    if is_self(i, dyl, dx):
                        pltpu.make_async_copy(source, target, self_sem.at[r]).start()
                    else:
                        to = device(tx, tyl, yh ^ dyh, (z + dz) % 4, core)
                        remote(source, target, back_send.at[r, i], back_recv.at[r, i], to).start()

    store_res = pltpu.make_async_copy(res_buf, resid, in_sem.at[0])
    store_res.start()
    store_tables.wait()
    for i in range(8):
        shares[i].wait_send()
        for r in range(2):
            remote(
                outgoing.at[r, i, pl.ds(0, KEPT[i])], incoming.at[r, i, pl.ds(0, KEPT[i])],
                send_sem.at[r, i], recv_sem.at[r, i],
            ).wait_send()
    passes = []
    for r in range(2):
        if r == 1:
            for i in range(8):
                remote(
                    gp.at[0, pl.ds(0, KEPT[i])], incoming.at[0, i, pl.ds(0, KEPT[i])],
                    back_send.at[0, i], back_recv.at[0, i],
                ).wait_send()
            for store in passes:
                store.wait()
            passes = []
        for i, (dz, dyh) in enumerate(ORDER):
            block = ((z + 4 - dz) % 4) * 2 + (yh ^ dyh)
            rows = gathered.at[block, :, r]
            count = 8
            if ORDER[i] == (0, 0):
                pltpu.make_async_copy(gp.at[r, 0], gathered.at[block, 0, r], self_sem.at[r]).wait()
                count = 7
            remote(
                gp.at[r, pl.ds(0, count)], gathered.at[block, pl.ds(0, count), r],
                back_send.at[r, i], back_recv.at[r, i],
            ).wait_recv()
            home = grad_rows.at[block, core, :, r]
            onward = remote(rows, home, share_send.at[r, i], share_recv.at[r, i])
            onward.start()
            store = pltpu.make_async_copy(rows, home, out_sem.at[r, i])
            store.start()
            passes += [onward, store]
    for store in passes + [store_res]:
        store.wait()
    for i in range(8):
        remote(
            gp.at[1, pl.ds(0, KEPT[i])], incoming.at[1, i, pl.ds(0, KEPT[i])], back_send.at[1, i], back_recv.at[1, i]
        ).wait_send()


def back_project(
    rows_hbm, tables_hbm, res_in, shift_hbm, grad, res_out,
    rows_ref, tables, res_buf, shift, staged, load_sem, small_sem, sem,
):
    words = pltpu.make_async_copy(shift_hbm, shift, small_sem.at[1])
    load_tables = pltpu.make_async_copy(tables_hbm, tables, small_sem.at[0])
    loads = [
        pltpu.make_async_copy(rows_hbm.at[pl.ds(low, size)], rows_ref.at[pl.ds(low, size)], load_sem.at[t])
        for t, (low, size) in enumerate(PIECES)
    ]
    last = pltpu.make_async_copy(res_in, res_buf, small_sem.at[2])
    for load in [load_tables, loads[0], words] + loads[1:] + [last]:
        load.start()
    load_tables.wait()
    stores = []
    for t, (low, size) in enumerate(PIECES):
        span = pl.ds(low, size)
        loads[t].wait()
        empty = jnp.zeros((size, HALF), jnp.bfloat16)
        windows = [jnp.concatenate([empty, rows_ref[span, :HALF]], axis=1)]
        windows += [rows_ref[span, q * HALF : q * HALF + BLOCK] for q in range(3)]
        windows += [jnp.concatenate([rows_ref[span, 3 * HALF :], empty], axis=1)]
        if t == 0:
            words.wait()
        for pair in range(LOCAL // 2):
            for n, window in enumerate(windows):
                wide = jnp.dot(window, tables[pair], preferred_element_type=jnp.float32).astype(jnp.bfloat16)
                for half in range(2):
                    staged[2 * pair + half, span, n * HALF : (n + 1) * HALF] = wide[:, half * HALF : (half + 1) * HALF]
            for layer in (2 * pair, 2 * pair + 1):
                first = pl.multiple_of(jnp.where(shift[layer] < 0, 0, HALF), HALF)
                store = pltpu.make_async_copy(
                    staged.at[layer, span, pl.ds(first, X)],
                    grad.at[layer, span],
                    sem.at[t * LOCAL + layer],
                )
                store.start()
                stores.append(store)
        if t == 0:
            last.wait()
            keep = pltpu.make_async_copy(res_buf, res_out, small_sem.at[0])
            keep.start()
            stores.append(keep)
    for store in stores:
        store.wait()


def shards(volume, shift, frac, basis, data, mask):
    layers, rows, coefs, cols = volume.shape
    flat = rows * coefs
    hbm = pl.BlockSpec(memory_space=pl.ANY)
    dma = pltpu.SemaphoreType.DMA
    tall = layers * BLOCK
    grad_rows, tables, resid = pl.pallas_call(
        exchange,
        out_shape=(
            jax.ShapeDtypeStruct((8, 2, 8, 2, coefs, cols), jnp.bfloat16),
            jax.ShapeDtypeStruct((layers // 2, BLOCK, BLOCK), jnp.bfloat16),
            jax.ShapeDtypeStruct(data.shape, jnp.bfloat16),
        ),
        in_specs=[hbm] * 6,
        out_specs=(hbm, hbm, hbm),
        scratch_shapes=[
            pltpu.VMEM((8, layers, BLOCK, cols), jnp.bfloat16),
            pltpu.SMEM(shift.shape, jnp.int32),
            pltpu.SMEM(frac.shape, jnp.int32),
            pltpu.VMEM((tall, BLOCK), jnp.bfloat16),
            pltpu.VMEM((tall, BLOCK), jnp.bfloat16),
            pltpu.VMEM((layers // 2, BLOCK, BLOCK), jnp.bfloat16),
            pltpu.VMEM((8, 8, 2, coefs, cols), jnp.bfloat16),
            pltpu.VMEM(data.shape, jnp.bfloat16),
            pltpu.VMEM((8, 2, 8, 2, coefs, cols), jnp.float32),
            pltpu.VMEM((8, 8, 2, coefs, cols), jnp.float32),
            pltpu.VMEM((2, 8, 8, coefs, cols), jnp.bfloat16),
            pltpu.VMEM((2, 8, 8, coefs, cols), jnp.bfloat16),
            pltpu.VMEM((2, 64, cols), jnp.float32),
            pltpu.VMEM(data.shape, jnp.float32),
            pltpu.VMEM(mask.shape, jnp.int32),
            pltpu.VMEM(basis.shape, jnp.bfloat16),
            pltpu.VMEM((2, 8, coefs, cols), jnp.bfloat16),
            dma((8,)), dma((5,)), dma((2,)), dma((8,)), dma((8,)), dma((2, 8)), dma((2, 8)),
            dma((2, 8)), dma((2, 8)), dma((2, 8)), dma((2, 8)), dma((2, 8)),
        ],
        compiler_params=pltpu.CompilerParams(collective_id=0, has_side_effects=True, vmem_limit_bytes=VMEM),
        name="exchange",
    )(volume.reshape(layers, flat, cols), shift, frac, basis, data, mask)
    gradient, residual = pl.pallas_call(
        back_project,
        out_shape=(
            jax.ShapeDtypeStruct((layers, flat, cols), jnp.bfloat16),
            jax.ShapeDtypeStruct(data.shape, jnp.bfloat16),
        ),
        in_specs=[hbm] * 4,
        out_specs=(hbm, hbm),
        scratch_shapes=[
            pltpu.VMEM((flat, cols), jnp.bfloat16),
            pltpu.VMEM((layers // 2, BLOCK, BLOCK), jnp.bfloat16),
            pltpu.VMEM(data.shape, jnp.bfloat16),
            pltpu.SMEM(shift.shape, jnp.int32),
            pltpu.VMEM((layers, flat, cols + HALF), jnp.bfloat16),
            dma((len(PIECES),)),
            dma((3,)),
            dma((len(PIECES) * layers,)),
        ],
        compiler_params=pltpu.CompilerParams(vmem_limit_bytes=VMEM),
        name="back_project",
    )(grad_rows.reshape(flat, cols), tables, resid, shift)
    return gradient.reshape(volume.shape), residual


def solution(mesh):
    in_specs = (
        P("depth", None, "coef", None),
        P("depth"),
        P("depth"),
        P(),
        P(("depth", "coef"), None, None),
        P(("depth", "coef"), None, None),
    )
    out_specs = (P("depth", None, "coef", None), P(("depth", "coef"), None, None))
    return jax.shard_map(shards, mesh=mesh, in_specs=in_specs, out_specs=out_specs, check_vma=False)
```
